512 devices in a mesh: dp: 32 (over x, y), expert: 16 (over z, core).
Axes of the slice: x: 4, y: 8, z: 8, core: 2. Of those that a mesh axis runs over, the one named last changes fastest.
Arguments:
- grad_out: bfloat16 [8192, 2048], P('dp', 'expert'), may hold values from -48 to 48
- saved_inputs: bfloat16 [8192, 2048], P('dp', 'expert'), may hold values from -6 to 6
- router_probs: float32 [16, 8192], P('expert', 'dp'), may hold values from 0 to 1, as said below
- chosen: int32 [16, 512], replicated, may hold values from 0 to 8191, as said below
- gate_pre: bfloat16 [16, 512, 7168], P('expert', None, 'dp'), may hold values from -6 to 6
- up_pre: bfloat16 [16, 512, 7168], P('expert', None, 'dp'), may hold values from -6 to 6
- w_down: bfloat16 [16, 7168, 2048], P('expert', 'dp'), may hold values from -0.0625 to 0.0625
- w_up: bfloat16 [16, 7168, 2048], P('expert', 'dp'), may hold values from -0.125 to 0.125
Outputs:
- grad_tokens: bfloat16 [8192, 2048], P('dp', 'expert')
- grad_logits: float32 [16, 8192], P('expert', 'dp')
- grad_down: bfloat16 [16, 7168, 2048], P('expert', 'dp')
- grad_up: bfloat16 [16, 7168, 2048], P('expert', 'dp')
- grad_gate_pre: bfloat16 [16, 512, 7168], P('expert', None, 'dp')
The draws below stay inside these ranges and needn't reach their ends.
Inputs may be any that keep to these rules, and one draw needn't show every extreme that they name: `chosen`: every row lists 512 different tokens in increasing order. Among the 256 consecutive tokens of one index of dp, an expert chooses at most 24, and every expert chooses exactly 24 from some index of dp. `router_probs`: each token's probabilities over the 16 experts are positive and sum to one.
All inputs are finite; a program needn't handle non-finite values.
Results may differ from the reference program's by a relative error of at most 0.04.
Values may be sent and summed in bfloat16 or wider, within the bound.
No kernel may reach another device: no remote copies, remote signals or barrier semaphores. Data moves between devices by JAX's collectives and lax.ppermute only.
A program may use at most 64 MiB of HBM per device.

```python
import jax
import jax.numpy as jnp
from jax import lax

WIDTH = 2048
FF_UNITS = 7168
TOK_DEV = 256
EXPERTS = 16
TOKENS = 8192
SLOTS = 512
CAP = 24
N_DP = 32


def draw_router_probs(key, part):
    first_key = jax.random.fold_in(key, 0)
    logits = 1.5 * jax.random.normal(first_key, (EXPERTS, TOKENS), jnp.float32)
    return jax.nn.softmax(logits, axis=0).astype(jnp.float32)


def draw_chosen(key, part):
    shard_total = TOKENS // TOK_DEV
    tier_key, top_key, noise_key = jax.random.split(key, 3)
    tiers = jax.random.randint(tier_key, (EXPERTS, shard_total), 0, 3)
    favored = jax.random.randint(top_key, (EXPERTS,), 0, shard_total)
    shard_ids = jnp.arange(shard_total, dtype=jnp.int32)
    tiers = jnp.where(shard_ids[None, :] == favored[:, None], 3, tiers)
    noise = jax.random.randint(noise_key, (EXPERTS, shard_total, TOK_DEV), 0, 4096)
    local_ids = jnp.arange(TOK_DEV, dtype=jnp.int32)
    distinct = noise * TOK_DEV + local_ids[None, None, :]
    order = jnp.argsort(-distinct, axis=2, stable=True)
    ranks = jnp.argsort(order, axis=2, stable=True)
    eligible = ranks < CAP
    global_ids = jnp.arange(TOKENS, dtype=jnp.int32).reshape(1, shard_total, TOK_DEV)
    scores = (tiers[:, :, None] * 4096 + noise) * TOKENS + global_ids
    scores = jnp.where(eligible, scores, -1).reshape(EXPERTS, TOKENS)
    picked = lax.top_k(scores, SLOTS)[1]
    return jnp.sort(picked, axis=1).astype(jnp.int32)


def block_scale(key, extent, cuts, smallest, top_value):
    def one(dim, parts):
        steps = jax.random.uniform(jax.random.fold_in(jax.random.fold_in(key, 6), dim), (parts,), jnp.float32, smallest / len(cuts), top_value / len(cuts))
        return jnp.repeat(jnp.exp(steps), extent[dim] // parts).reshape((-1,) + (1,) * (len(extent) - dim - 1))

    factor_of = one(*cuts[0])
    for cut in cuts[1:]:
        factor_of = factor_of * one(*cut)
    return factor_of


def gaussian(key, extent, spread, reach, cuts=(), held_as=jnp.bfloat16):
    drawn = spread * jax.random.normal(key, extent, jnp.float32)
    if cuts:
        drawn = drawn * block_scale(key, extent, cuts, -0.22, 0.18)
    return jnp.clip(drawn, -reach, reach).astype(held_as)


def setup_inputs(seed: int = 0) -> dict:
    arg_keys = jax.random.split(jax.random.key(seed), 9)
    return {
        "grad_out": gaussian(arg_keys[0], (TOKENS, WIDTH), 8.0, 48.0, ((0, 32), (1, 16))),
        "saved_inputs": gaussian(arg_keys[1], (TOKENS, WIDTH), 1.0, 6.0, ((0, 32), (1, 16))),
        "router_probs": draw_router_probs(jax.random.fold_in(arg_keys[8], 71), 0),
        "chosen": draw_chosen(jax.random.fold_in(arg_keys[8], 71), 0),
        "gate_pre": gaussian(arg_keys[4], (EXPERTS, SLOTS, FF_UNITS), 1.0, 6.0, ((0, 16), (2, 32))),
        "up_pre": gaussian(arg_keys[5], (EXPERTS, SLOTS, FF_UNITS), 1.0, 6.0, ((0, 16), (2, 32))),
        "w_down": gaussian(arg_keys[6], (EXPERTS, FF_UNITS, WIDTH), FF_UNITS ** -0.5, 0.0625, ((0, 16), (1, 32))),
        "w_up": gaussian(arg_keys[7], (EXPERTS, FF_UNITS, WIDTH), WIDTH ** -0.5, 0.125, ((0, 16), (1, 32))),
    }


def expert_backward(operands):
    dout_rows, input_rows, gate_slot, gate_block, up_block, down_block, upw_block = operands
    gate_value = gate_block.astype(jnp.float32)
    up_value = up_block.astype(jnp.float32)
    sigmoid_gate = jax.nn.sigmoid(gate_value)
    active = gate_value * sigmoid_gate
    hidden = active * up_value
    raw_grad = lax.dot_general(dout_rows, down_block, (((1,), (1,)), ((), ())), preferred_element_type=jnp.float32)
    hid_grad = gate_slot.astype(jnp.float32)[:, None] * raw_grad
    up_grad = (hid_grad * active).astype(jnp.bfloat16)
    gate_grad = (hid_grad * up_value * sigmoid_gate * (1.0 + gate_value * (1.0 - sigmoid_gate))).astype(jnp.bfloat16)
    out_grad = gate_slot[:, None] * dout_rows
    grad_down = lax.dot_general(hidden.astype(jnp.bfloat16), out_grad, (((0,), (0,)), ((), ())), preferred_element_type=jnp.float32).astype(jnp.bfloat16)
    grad_up = lax.dot_general(up_grad, input_rows, (((0,), (0,)), ((), ())), preferred_element_type=jnp.float32).astype(jnp.bfloat16)
    unit_block = FF_UNITS // N_DP
    up_split = up_grad.astype(jnp.float32).reshape(SLOTS, N_DP, unit_block)
    weight_split = upw_block.astype(jnp.float32).reshape(N_DP, unit_block, WIDTH)
    partial_value = jnp.einsum("spu,puw->psw", up_split, weight_split, precision=lax.Precision.HIGHEST)
    rounded = lax.optimization_barrier(partial_value.astype(jnp.bfloat16))
    expert_dx = jnp.sum(rounded.astype(jnp.float32), axis=0)
    dot_split = jnp.sum((hidden * raw_grad).reshape(SLOTS, N_DP, unit_block), axis=2)
    dot_round = lax.optimization_barrier(dot_split.astype(jnp.bfloat16))
    slot_dots = jnp.sum(dot_round.astype(jnp.float32), axis=1)
    return expert_dx, slot_dots, grad_down, grad_up, gate_grad


def reference(grad_out, saved_inputs, router_probs, chosen, gate_pre, up_pre, w_down, w_up):
    dout_rows = grad_out[chosen]
    input_rows = saved_inputs[chosen]
    gate_slot = jnp.take_along_axis(router_probs, chosen, axis=1).astype(jnp.bfloat16)
    results = lax.map(expert_backward, (dout_rows, input_rows, gate_slot, gate_pre, up_pre, w_down, w_up))
    expert_dx, slot_dots, grad_down, grad_up, grad_gate_pre = results
    summed = jax.ops.segment_sum(expert_dx.reshape(-1, WIDTH), chosen.reshape(-1), num_segments=TOKENS)
    grad_tokens = summed.astype(jnp.bfloat16)
    expert_ids = jnp.arange(EXPERTS, dtype=jnp.int32)[:, None]
    gate_grad = jnp.zeros((EXPERTS, TOKENS), jnp.float32).at[expert_ids, chosen].set(slot_dots)
    router_sum = jnp.sum(router_probs * gate_grad, axis=0)
    grad_logits = router_probs * (gate_grad - router_sum[None, :])
    return grad_tokens, grad_logits, grad_down, grad_up, grad_gate_pre
```

```python
import jax
import jax.numpy as jnp
from jax import lax
from jax.sharding import Mesh
from jax.sharding import PartitionSpec as P

X, Y, E = "dp_0", "dp_1", "expert"
BF, F32 = jnp.bfloat16, jnp.float32
PAD = 8


def exchange(x, axis):
    return lax.all_to_all(x, axis, 0, 0, tiled=True)


def to_all(x, axis):
    size = lax.axis_size(axis)
    return exchange(jnp.broadcast_to(x[None], (size, *x.shape)), axis)


def dot(a, b, ca, cb):
    return lax.dot_general(a, b, (((ca,), (cb,)), ((), ())), preferred_element_type=F32)


def onehot(mask):
    return mask.astype(BF)


def rows_of(n, m):
    return lax.broadcasted_iota(jnp.int32, (n, m), 0)


def lanes_of(n, m):
    return lax.broadcasted_iota(jnp.int32, (n, m), 1)


def features_to_x(w, nx):
    units, width = w.shape
    parts = w.reshape(units, nx, width // nx).transpose(1, 0, 2)
    return exchange(parts, X).reshape(nx * units, width // nx)


def features_home(g, nx):
    parts = exchange(g.reshape(nx, g.shape[0] // nx, g.shape[1]), X)
    return parts.transpose(1, 0, 2).reshape(parts.shape[1], -1)


def local(grad_out, saved_inputs, router_probs, chosen, gate_pre, up_pre, w_down, w_up):
    tok_dev, width_dev = grad_out.shape
    nx, ny, ne = lax.axis_size(X), lax.axis_size(Y), lax.axis_size(E)
    shards = nx * ny
    xi, yi, ei = lax.axis_index(X), lax.axis_index(Y), lax.axis_index(E)
    shard = xi * ny + yi
    slots = chosen.shape[1]
    cap = 3 * slots // (2 * shards)
    units = gate_pre.shape[2]
    quarter = ne // nx
    part = quarter * width_dev
    lane = 128

    firsts = jnp.sum((chosen < shard * tok_dev).astype(jnp.int32), axis=1)
    ends = jnp.sum((chosen < (shard + 1) * tok_dev).astype(jnp.int32), axis=1)
    offsets = jnp.arange(cap + PAD, dtype=jnp.int32)
    places = firsts[:, None] + offsets[None, :]
    live = (places < ends[:, None]) & (offsets < cap)[None, :]
    slot_iota = jnp.arange(slots, dtype=jnp.int32)
    found = jnp.sum(
        jnp.where(places[:, :, None] == slot_iota[None, None, :], chosen[:, None, :], 0), axis=2
    )
    local_rows = jnp.where(live, found - shard * tok_dev, -1)
    token_iota = jnp.arange(tok_dev, dtype=jnp.int32)
    picker = onehot(local_rows[:, :, None] == token_iota[None, None, :])

    flat_pick = picker.reshape(ne * (cap + PAD), tok_dev)
    sent_grad = dot(flat_pick, grad_out, 1, 0).astype(BF).reshape(ne, cap + PAD, width_dev)
    sent_input = dot(flat_pick, saved_inputs, 1, 0).astype(BF).reshape(ne, cap + PAD, width_dev)
    sent = jnp.concatenate([sent_grad[:, :cap], sent_input[:, :cap]], axis=1)
    rows = exchange(sent, E).reshape(nx, quarter, 2 * cap, width_dev)

    down_part = features_to_x(w_down[0], nx)
    up_part = features_to_x(w_up[0], nx)

    own_rows = lax.dynamic_index_in_dim(local_rows, ei, 0, keepdims=False)
    own_rows = jnp.pad(own_rows, (0, lane - cap - PAD), constant_values=-1)
    own_hit = onehot(own_rows[:, None] == token_iota[None, :])
    gate_row = dot(router_probs.astype(BF), own_hit, 1, 1).astype(BF)
    gate_tile = jnp.broadcast_to(
        jnp.pad(gate_row, ((0, PAD - 1), (0, 0)))[None, None], (nx, quarter, PAD, lane)
    )
    rows = exchange(jnp.concatenate([rows, gate_tile], axis=2), X)
    grads = rows[:, :, :cap].transpose(0, 2, 1, 3).reshape(nx * cap, part)
    inputs = rows[:, :, cap : 2 * cap].transpose(0, 2, 1, 3).reshape(nx * cap, part)
    gates = jnp.pad(rows[:, 0, 2 * cap], ((0, PAD - nx), (0, part - lane)))
    block = nx * cap + PAD
    grads_all = to_all(jnp.concatenate([grads, gates], axis=0), Y)
    inputs_all = to_all(inputs, Y)

    chosen_row = lax.dynamic_index_in_dim(chosen, ei, 0, keepdims=True)
    owner = chosen_row // tok_dev
    shard_col = rows_of(shards, slots)
    before = jnp.sum((owner < shard_col).astype(jnp.int32), axis=1, keepdims=True)
    within = lanes_of(1, slots) - jnp.sum(
        jnp.where(owner == shard_col, before, 0), axis=0, keepdims=True
    )
    owner_x, owner_y = owner // ny, owner % ny
    spot = owner_x * cap + within
    place_block = onehot(rows_of(ny * block, slots) == owner_y * block + spot)
    place_rows = onehot(rows_of(ny * nx * cap, slots) == owner_y * (nx * cap) + spot)
    owner_hit = rows_of(shards, slots) == owner_y * nx + owner_x
    within_hit = onehot(rows_of(lane, slots) == within)

    gate_value = gate_pre[0].T.astype(F32)
    up_value = up_pre[0].T.astype(F32)
    sig = jax.nn.sigmoid(gate_value)
    active = gate_value * sig
    hidden = active * up_value
    hidden_all = to_all(hidden.astype(BF), X).reshape(nx * units, slots)

    grads_slots = dot(place_block, grads_all.reshape(ny * block, part), 0, 0).astype(BF)
    gates_all = grads_all[:, nx * cap : nx * cap + nx, :lane].reshape(shards, lane)
    gate_slot = jnp.sum(
        jnp.where(owner_hit, dot(gates_all, within_hit, 1, 0), 0.0), axis=0, keepdims=True
    )
    raw_part = dot(down_part, grads_slots, 1, 1).astype(BF).reshape(nx, units, slots)
    raw_grad = jnp.sum(exchange(raw_part, X).astype(F32), axis=0)
    dots = jnp.sum(hidden * raw_grad, axis=0, keepdims=True)
    hid_grad = gate_slot * raw_grad
    up_grad = (hid_grad * active).astype(BF)
    gate_grad = (hid_grad * up_value * sig * (1.0 + gate_value * (1.0 - sig))).astype(BF)
    up_all = to_all(up_grad, X).reshape(nx * units, slots)

    dx = dot(up_all, up_part, 0, 0).astype(BF)
    dx_rows = dot(place_rows, dx, 1, 0).astype(BF).reshape(ny, nx * cap, part)
    dots_own = jnp.where(owner_hit, dots, 0.0).astype(BF)
    dots_rows = dot(dots_own, within_hit, 1, 1).astype(BF).reshape(ny, nx, lane)
    dots_rows = jnp.pad(dots_rows, ((0, 0), (0, PAD - nx), (0, part - lane)))
    dx_back = exchange(jnp.concatenate([dx_rows, dots_rows], axis=1), Y)
    dx_sum = jnp.sum(dx_back.astype(F32), axis=0).astype(BF)
    dots_sum = dx_sum[nx * cap : nx * cap + nx].reshape(nx, 1, part)
    dx_sum = jnp.concatenate(
        [dx_sum[: nx * cap].reshape(nx, cap, part), jnp.pad(dots_sum, ((0, 0), (0, PAD - 1), (0, 0)))],
        axis=1,
    )
    dx_own = exchange(dx_sum, X)
    gate_tokens = jnp.sum(dot(dx_own[:, cap, :lane], own_hit, 1, 0), axis=0, keepdims=True)
    product = router_probs * gate_tokens
    high = lax.reduce_precision(product, 8, 7)
    low = product - high
    tail = jnp.concatenate([high, low], axis=0).astype(BF).reshape(-1, lane)
    tail = jnp.pad(tail, ((0, PAD - tail.shape[0]), (0, 0)))
    to_experts = dx_own[:, :cap].reshape(nx, cap, quarter, width_dev).transpose(0, 2, 1, 3)
    to_experts = to_experts.reshape(ne, cap, width_dev)
    spread = exchange(
        jnp.concatenate([to_experts, jnp.broadcast_to(tail[None], (ne, PAD, lane))], axis=1), E
    )
    grad_tokens = dot(flat_pick, spread.reshape(-1, width_dev), 0, 0).astype(BF)
    pieces = jnp.sum(spread[:, cap : cap + 2 * tok_dev // lane].astype(F32), axis=0)
    router_sum = jnp.sum(pieces.reshape(2, 1, tok_dev), axis=0)
    grad_logits = router_probs * (gate_tokens - router_sum)

    hidden_gated = (hidden_all.astype(F32) * gate_slot).astype(BF)
    grad_down = dot(hidden_gated, grads_slots, 1, 0).astype(BF)
    inputs_slots = dot(place_rows, inputs_all.reshape(-1, part), 0, 0).astype(BF)
    grad_up = dot(up_all, inputs_slots, 1, 0).astype(BF)
    grad_down = features_home(grad_down, nx)
    grad_up = features_home(grad_up, nx)
    return grad_tokens, grad_logits, grad_down[None], grad_up[None], gate_grad.T[None]


def solution(mesh):
    split = Mesh(mesh.devices.reshape(4, 8, mesh.shape["expert"]), (X, Y, E))
    dp = (X, Y)
    return jax.shard_map(
        local,
        mesh=split,
        in_specs=(
            P(dp, E),
            P(dp, E),
            P(E, dp),
            P(),
            P(E, None, dp),
            P(E, None, dp),
            P(E, dp, None),
            P(E, dp, None),
        ),
        out_specs=(P(dp, E), P(E, dp), P(E, dp, None), P(E, dp, None), P(E, None, dp)),
        check_vma=False,
    )
```

```python
import jax
import jax.numpy as jnp
from jax import lax
from jax.sharding import Mesh
from jax.sharding import PartitionSpec as P


X, Y, E = "dp_0", "dp_1", "expert"
BF, F32 = jnp.bfloat16, jnp.float32
PAD = 8


def exchange(x, axis):
    return lax.all_to_all(x, axis, 0, 0, tiled=True)


def to_all(x, axis):
    size = lax.axis_size(axis)
    return exchange(jnp.broadcast_to(x[None], (size, *x.shape)), axis)


def dot(a, b, ca, cb):
    return lax.dot_general(a, b, (((ca,), (cb,)), ((), ())), preferred_element_type=F32)


def onehot(mask):
    return mask.astype(BF)


def rows_of(n, m):
    return lax.broadcasted_iota(jnp.int32, (n, m), 0)


def lanes_of(n, m):
    return lax.broadcasted_iota(jnp.int32, (n, m), 1)


def shift(x, by):
    size = lax.axis_size(X)
    return lax.ppermute(x, X, [(i, (i + by) % size) for i in range(size)])


def quarter_at(w, index, nx):
    return lax.dynamic_slice_in_dim(w, index * (w.shape[1] // nx), w.shape[1] // nx, axis=1)


def in_turn(parts, xi):
    size = len(parts)
    stacked = jnp.stack(parts)
    picked = [
        lax.dynamic_index_in_dim(stacked, (q + size - xi) % size, 0, keepdims=False)
        for q in range(size)
    ]
    return jnp.concatenate(picked, axis=1)


def local(grad_out, saved_inputs, router_probs, chosen, gate_pre, up_pre, w_down, w_up):
    tok_dev, width_dev = grad_out.shape
    nx, ny, ne = lax.axis_size(X), lax.axis_size(Y), lax.axis_size(E)
    shards = nx * ny
    xi, yi, ei = lax.axis_index(X), lax.axis_index(Y), lax.axis_index(E)
    shard = xi * ny + yi
    slots = chosen.shape[1]
    cap = 3 * slots // (2 * shards)
    units = gate_pre.shape[2]
    quarter = ne // nx
    part = quarter * width_dev
    lane = 128

    firsts = jnp.sum((chosen < shard * tok_dev).astype(jnp.int32), axis=1)
    ends = jnp.sum((chosen < (shard + 1) * tok_dev).astype(jnp.int32), axis=1)
    offsets = jnp.arange(cap + PAD, dtype=jnp.int32)
    places = firsts[:, None] + offsets[None, :]
    live = (places < ends[:, None]) & (offsets < cap)[None, :]
    slot_iota = jnp.arange(slots, dtype=jnp.int32)
    found = jnp.sum(
        jnp.where(places[:, :, None] == slot_iota[None, None, :], chosen[:, None, :], 0), axis=2
    )
    local_rows = jnp.where(live, found - shard * tok_dev, -1)
    token_iota = jnp.arange(tok_dev, dtype=jnp.int32)
    picker = onehot(local_rows[:, :, None] == token_iota[None, None, :])

    flat_pick = picker.reshape(ne * (cap + PAD), tok_dev)
    sent_grad = dot(flat_pick, grad_out, 1, 0).astype(BF).reshape(ne, cap + PAD, width_dev)
    sent_input = dot(flat_pick, saved_inputs, 1, 0).astype(BF).reshape(ne, cap + PAD, width_dev)
    sent = jnp.concatenate([sent_grad[:, :cap], sent_input[:, :cap]], axis=1)
    rows = exchange(sent, E).reshape(nx, quarter, 2 * cap, width_dev)

    down_mine = [quarter_at(w_down[0], (xi + k) % nx, nx) for k in range(nx)]
    up_mine = [quarter_at(w_up[0], (xi + k) % nx, nx) for k in range(nx)]
    down_part = jnp.concatenate(
        [down_mine[0]] + [shift(down_mine[k], k) for k in range(1, nx)], axis=0
    )

    own_rows = lax.dynamic_index_in_dim(local_rows, ei, 0, keepdims=False)
    own_rows = jnp.pad(own_rows, (0, lane - cap - PAD), constant_values=-1)
    own_hit = onehot(own_rows[:, None] == token_iota[None, :])
    gate_row = dot(router_probs.astype(BF), own_hit, 1, 1).astype(BF)
    gate_tile = jnp.broadcast_to(
        jnp.pad(gate_row, ((0, PAD - 1), (0, 0)))[None, None], (nx, quarter, PAD, lane)
    )
    rows = exchange(jnp.concatenate([rows, gate_tile], axis=2), X)
    gate_value = gate_pre[0].T.astype(F32)
    up_value = up_pre[0].T.astype(F32)
    sig = jax.nn.sigmoid(gate_value)
    active = gate_value * sig
    hidden = active * up_value
    hidden_own = hidden.astype(BF)
    up_mine, hidden_own, rows, down_part = lax.optimization_barrier(
        (up_mine, hidden_own, rows, down_part)
    )
    pairs = [
        shift(jnp.concatenate([up_mine[k], hidden_own], axis=0), k) for k in range(1, nx)
    ]
    up_part = jnp.concatenate([up_mine[0]] + [p[:units] for p in pairs], axis=0)
    hidden_all = jnp.concatenate([hidden_own] + [p[units:] for p in pairs], axis=0)

    grads = rows[:, :, :cap].transpose(0, 2, 1, 3).reshape(nx * cap, part)
    inputs = rows[:, :, cap : 2 * cap].transpose(0, 2, 1, 3).reshape(nx * cap, part)
    gates = jnp.pad(rows[:, 0, 2 * cap], ((0, PAD - nx), (0, part - lane)))
    block = nx * cap + PAD
    grads_all = to_all(jnp.concatenate([grads, gates], axis=0), Y)

    chosen_row = lax.dynamic_index_in_dim(chosen, ei, 0, keepdims=True)
    owner = chosen_row // tok_dev
    shard_col = rows_of(shards, slots)
    before = jnp.sum((owner < shard_col).astype(jnp.int32), axis=1, keepdims=True)
    within = lanes_of(1, slots) - jnp.sum(
        jnp.where(owner == shard_col, before, 0), axis=0, keepdims=True
    )
    owner_x, owner_y = owner // ny, owner % ny
    spot = owner_x * cap + within
    place_block = onehot(rows_of(ny * block, slots) == owner_y * block + spot)
    place_rows = onehot(rows_of(ny * nx * cap, slots) == owner_y * (nx * cap) + spot)
    owner_hit = rows_of(shards, slots) == owner_y * nx + owner_x
    within_hit = onehot(rows_of(lane, slots) == within)

    grads_all, up_part, hidden_all = lax.optimization_barrier((grads_all, up_part, hidden_all))
    grads_slots = dot(place_block, grads_all.reshape(ny * block, part), 0, 0).astype(BF)
    gates_all = grads_all[:, nx * cap : nx * cap + nx, :lane].reshape(shards, lane)
    gate_slot = jnp.sum(
        jnp.where(owner_hit, dot(gates_all, within_hit, 1, 0), 0.0), axis=0, keepdims=True
    )
    raw_part = dot(down_part, grads_slots, 1, 1).astype(BF).reshape(nx, units, slots)
    inputs, raw_part = lax.optimization_barrier((inputs, raw_part))
    inputs_all = to_all(inputs, Y)
    raw_came = [shift(raw_part[k], -k) for k in range(1, nx)]
    raw_grad = raw_part[0].astype(F32)
    for came in raw_came:
        raw_grad = raw_grad + came.astype(F32)
    dots = jnp.sum(hidden * raw_grad, axis=0, keepdims=True)
    hid_grad = gate_slot * raw_grad
    up_grad = (hid_grad * active).astype(BF)
    gate_grad = (hid_grad * up_value * sig * (1.0 + gate_value * (1.0 - sig))).astype(BF)
    up_all = jnp.concatenate([up_grad] + [shift(up_grad, k) for k in range(1, nx)], axis=0)

    dx = dot(up_all, up_part, 0, 0).astype(BF)
    dx_rows = dot(place_rows, dx, 1, 0).astype(BF).reshape(ny, nx * cap, part)
    dots_own = jnp.where(owner_hit, dots, 0.0).astype(BF)
    dots_rows = dot(dots_own, within_hit, 1, 1).astype(BF).reshape(ny, nx, lane)
    dots_rows = jnp.pad(dots_rows, ((0, 0), (0, PAD - nx), (0, part - lane)))
    dx_back = exchange(jnp.concatenate([dx_rows, dots_rows], axis=1), Y)
    dx_sum = jnp.sum(dx_back.astype(F32), axis=0).astype(BF)
    dots_sum = dx_sum[nx * cap : nx * cap + nx].reshape(nx, 1, part)
    dx_sum = jnp.concatenate(
        [dx_sum[: nx * cap].reshape(nx, cap, part), jnp.pad(dots_sum, ((0, 0), (0, PAD - 1), (0, 0)))],
        axis=1,
    )
    dx_own = exchange(dx_sum, X)
    gate_tokens = jnp.sum(dot(dx_own[:, cap, :lane], own_hit, 1, 0), axis=0, keepdims=True)
    product = router_probs * gate_tokens
    high = lax.reduce_precision(product, 8, 7)
    low = product - high
    tail = jnp.concatenate([high, low], axis=0).astype(BF).reshape(-1, lane)
    tail = jnp.pad(tail, ((0, PAD - tail.shape[0]), (0, 0)))
    to_experts = dx_own[:, :cap].reshape(nx, cap, quarter, width_dev).transpose(0, 2, 1, 3)
    to_experts = to_experts.reshape(ne, cap, width_dev)
    spread = exchange(
        jnp.concatenate([to_experts, jnp.broadcast_to(tail[None], (ne, PAD, lane))], axis=1), E
    )
    grad_tokens = dot(flat_pick, spread.reshape(-1, width_dev), 0, 0).astype(BF)
    pieces = jnp.sum(spread[:, cap : cap + 2 * tok_dev // lane].astype(F32), axis=0)
    router_sum = jnp.sum(pieces.reshape(2, 1, tok_dev), axis=0)
    grad_logits = router_probs * (gate_tokens - router_sum)

    hidden_gated = (hidden_all.astype(F32) * gate_slot).astype(BF)
    grad_down = dot(hidden_gated, grads_slots, 1, 0).astype(BF)
    inputs_slots = dot(place_rows, inputs_all.reshape(-1, part), 0, 0).astype(BF)
    grad_up = dot(up_all, inputs_slots, 1, 0).astype(BF)
    both = jnp.concatenate(
        [grad_down.reshape(nx, units, part), grad_up.reshape(nx, units, part)], axis=1
    )
    home = [both[0]] + [shift(both[k], -k) for k in range(1, nx)]
    grad_down = in_turn([h[:units] for h in home], xi)
    grad_up = in_turn([h[units:] for h in home], xi)
    return grad_tokens, grad_logits, grad_down[None], grad_up[None], gate_grad.T[None]


def solution(mesh):
    split = Mesh(mesh.devices.reshape(4, 8, mesh.shape["expert"]), (X, Y, E))
    dp = (X, Y)
    return jax.shard_map(
        local,
        mesh=split,
        in_specs=(
            P(dp, E),
            P(dp, E),
            P(E, dp),
            P(),
            P(E, None, dp),
            P(E, None, dp),
            P(E, dp, None),
            P(E, dp, None),
        ),
        out_specs=(P(dp, E), P(E, dp), P(E, dp, None), P(E, dp, None), P(E, None, dp)),
        check_vma=False,
    )
```

```python
import jax
import jax.numpy as jnp
from jax import lax
from jax.sharding import Mesh
from jax.sharding import PartitionSpec as P


X, Y, E = "dp_0", "dp_1", "expert"
BF, F32 = jnp.bfloat16, jnp.float32
PAD = 8


def exchange(x, axis):
    return lax.all_to_all(x, axis, 0, 0, tiled=True)


def to_all(x, axis):
    size = lax.axis_size(axis)
    return exchange(jnp.broadcast_to(x[None], (size, *x.shape)), axis)


def dot(a, b, ca, cb):
    return lax.dot_general(a, b, (((ca,), (cb,)), ((), ())), preferred_element_type=F32)


def onehot(mask):
    return mask.astype(BF)


def rows_of(n, m):
    return lax.broadcasted_iota(jnp.int32, (n, m), 0)


def lanes_of(n, m):
    return lax.broadcasted_iota(jnp.int32, (n, m), 1)


def shift(x, by):
    size = lax.axis_size(X)
    return lax.ppermute(x, X, [(i, (i + by) % size) for i in range(size)])


def over_x(blocks, sign):
    came = [blocks[0]]
    for k in range(1, len(blocks)):
        came.append(shift(blocks[k], sign * k))
    return came


def back_in_x(blocks, xi):
    size = blocks.shape[0]
    return [
        lax.dynamic_index_in_dim(blocks, (xi + size - k) % size, 0, keepdims=False)
        for k in range(size)
    ]


def quarter_at(w, index, nx):
    return lax.dynamic_slice_in_dim(w, index * (w.shape[1] // nx), w.shape[1] // nx, axis=1)


def in_turn(parts, xi):
    size = len(parts)
    stacked = jnp.stack(parts)
    picked = [
        lax.dynamic_index_in_dim(stacked, (q + size - xi) % size, 0, keepdims=False)
        for q in range(size)
    ]
    return jnp.concatenate(picked, axis=1)


def local(grad_out, saved_inputs, router_probs, chosen, gate_pre, up_pre, w_down, w_up):
    tok_dev, width_dev = grad_out.shape
    nx, ny, ne = lax.axis_size(X), lax.axis_size(Y), lax.axis_size(E)
    shards = nx * ny
    xi, yi, ei = lax.axis_index(X), lax.axis_index(Y), lax.axis_index(E)
    shard = xi * ny + yi
    slots = chosen.shape[1]
    cap = 3 * slots // (2 * shards)
    units = gate_pre.shape[2]
    quarter = ne // nx
    part = quarter * width_dev
    lane = 128

    firsts = jnp.sum((chosen < shard * tok_dev).astype(jnp.int32), axis=1)
    ends = jnp.sum((chosen < (shard + 1) * tok_dev).astype(jnp.int32), axis=1)
    offsets = jnp.arange(cap + PAD, dtype=jnp.int32)
    places = firsts[:, None] + offsets[None, :]
    live = (places < ends[:, None]) & (offsets < cap)[None, :]
    slot_iota = jnp.arange(slots, dtype=jnp.int32)
    found = jnp.sum(
        jnp.where(places[:, :, None] == slot_iota[None, None, :], chosen[:, None, :], 0), axis=2
    )
    local_rows = jnp.where(live, found - shard * tok_dev, -1)
    token_iota = jnp.arange(tok_dev, dtype=jnp.int32)
    picker = onehot(local_rows[:, :, None] == token_iota[None, None, :])

    flat_pick = picker.reshape(ne * (cap + PAD), tok_dev)
    sent_grad = dot(flat_pick, grad_out, 1, 0).astype(BF).reshape(ne, cap + PAD, width_dev)
    sent_input = dot(flat_pick, saved_inputs, 1, 0).astype(BF).reshape(ne, cap + PAD, width_dev)
    sent = jnp.concatenate([sent_grad[:, :cap], sent_input[:, :cap]], axis=1)
    rows = exchange(sent, E)
    rows = rows.reshape(nx, quarter, 2 * cap, width_dev)

    down_part = jnp.concatenate([quarter_at(w_down[0], (xi + nx - k) % nx, nx) for k in range(nx)], axis=1)
    up_part = [quarter_at(w_up[0], (xi + k) % nx, nx) for k in range(nx)]
    up_part = jnp.concatenate(over_x(up_part, 1), axis=0)

    own_rows = lax.dynamic_index_in_dim(local_rows, ei, 0, keepdims=False)
    own_rows = jnp.pad(own_rows, (0, lane - cap - PAD), constant_values=-1)
    own_hit = onehot(own_rows[:, None] == token_iota[None, :])
    gate_row = dot(router_probs.astype(BF), own_hit, 1, 1).astype(BF)
    gate_tile = jnp.broadcast_to(
        jnp.pad(gate_row, ((0, PAD - 1), (0, 0)))[None, None], (nx, quarter, PAD, lane)
    )
    rows = exchange(jnp.concatenate([rows, gate_tile], axis=2), X)
    gate_value = gate_pre[0].T.astype(F32)
    up_value = up_pre[0].T.astype(F32)
    sig = jax.nn.sigmoid(gate_value)
    active = gate_value * sig
    hidden = active * up_value

    grads = rows[:, :, :cap].transpose(0, 2, 1, 3).reshape(nx * cap, part)
    inputs = rows[:, :, cap : 2 * cap].transpose(0, 2, 1, 3).reshape(nx * cap, part)
    gates = jnp.pad(rows[:, 0, 2 * cap], ((0, PAD - nx), (0, part - lane)))
    block = nx * cap + PAD
    grads_all = to_all(jnp.concatenate([grads, gates], axis=0), Y)
    inputs_all = to_all(inputs, Y)

    chosen_row = lax.dynamic_index_in_dim(chosen, ei, 0, keepdims=True)
    owner = chosen_row // tok_dev
    shard_col = rows_of(shards, slots)
    before = jnp.sum((owner < shard_col).astype(jnp.int32), axis=1, keepdims=True)
    within = lanes_of(1, slots) - jnp.sum(
        jnp.where(owner == shard_col, before, 0), axis=0, keepdims=True
    )
    owner_x, owner_y = owner // ny, owner % ny
    spot = owner_x * cap + within
    place_block = onehot(rows_of(ny * block, slots) == owner_y * block + spot)
    place_rows = onehot(rows_of(ny * nx * cap, slots) == owner_y * (nx * cap) + spot)
    owner_hit = rows_of(shards, slots) == owner_y * nx + owner_x
    within_hit = onehot(rows_of(lane, slots) == within)

    grads_slots = dot(place_block, grads_all.reshape(ny * block, part), 0, 0).astype(BF)
    gates_all = grads_all[:, nx * cap : nx * cap + nx, :lane].reshape(shards, lane)
    gate_slot = jnp.sum(
        jnp.where(owner_hit, dot(gates_all, within_hit, 1, 0), 0.0), axis=0, keepdims=True
    )
    grads_slots = jnp.concatenate(over_x([grads_slots] * nx, 1), axis=1)
    raw_grad = dot(down_part, grads_slots, 1, 1)
    dots = jnp.sum(hidden * raw_grad, axis=0, keepdims=True)
    hid_grad = gate_slot * raw_grad
    up_grad = (hid_grad * active).astype(BF)
    gate_grad = (hid_grad * up_value * sig * (1.0 + gate_value * (1.0 - sig))).astype(BF)
    up_all = lax.all_gather(up_grad, X)
    up_all = jnp.concatenate(back_in_x(up_all, xi), axis=0)

    hidden_gated = (hidden.astype(BF).astype(F32) * gate_slot).astype(BF)
    grad_down = dot(hidden_gated, grads_slots, 1, 0).astype(BF)
    grad_down = jnp.concatenate(
        [quarter_at(grad_down, (xi + nx - q) % nx, nx) for q in range(nx)], axis=1
    )
    dx = dot(up_all, up_part, 0, 0).astype(BF)
    dx_rows = dot(place_rows, dx, 1, 0).astype(BF).reshape(ny, nx * cap, part)
    dots_own = jnp.where(owner_hit, dots, 0.0).astype(BF)
    dots_rows = dot(dots_own, within_hit, 1, 1).astype(BF).reshape(ny, nx, lane)
    dots_rows = jnp.pad(dots_rows, ((0, 0), (0, PAD - nx), (0, part - lane)))
    dx_back = exchange(jnp.concatenate([dx_rows, dots_rows], axis=1), Y)
    inputs_slots = dot(place_rows, inputs_all.reshape(-1, part), 0, 0).astype(BF)
    grad_up = dot(up_all, inputs_slots, 1, 0).astype(BF).reshape(nx, units, part)
    up_home = over_x(grad_up, -1)
    dx_sum = jnp.sum(dx_back.astype(F32), axis=0).astype(BF)
    dots_sum = dx_sum[nx * cap : nx * cap + nx].reshape(nx, 1, part)
    dx_sum = jnp.concatenate(
        [dx_sum[: nx * cap].reshape(nx, cap, part), jnp.pad(dots_sum, ((0, 0), (0, PAD - 1), (0, 0)))],
        axis=1,
    )
    dx_own = exchange(dx_sum, X)
    gate_tokens = jnp.sum(dot(dx_own[:, cap, :lane], own_hit, 1, 0), axis=0, keepdims=True)
    product = router_probs * gate_tokens
    high = lax.reduce_precision(product, 8, 7)
    low = product - high
    tail = jnp.concatenate([high, low], axis=0).astype(BF).reshape(-1, lane)
    tail = jnp.pad(tail, ((0, PAD - tail.shape[0]), (0, 0)))
    to_experts = dx_own[:, :cap].reshape(nx, cap, quarter, width_dev).transpose(0, 2, 1, 3)
    to_experts = to_experts.reshape(ne, cap, width_dev)
    spread = exchange(
        jnp.concatenate([to_experts, jnp.broadcast_to(tail[None], (ne, PAD, lane))], axis=1), E
    )
    up_home, spread = lax.optimization_barrier((up_home, spread))
    grad_up = in_turn(up_home, xi)
    grad_tokens = dot(flat_pick, spread.reshape(-1, width_dev), 0, 0).astype(BF)
    pieces = jnp.sum(spread[:, cap : cap + 2 * tok_dev // lane].astype(F32), axis=0)
    router_sum = jnp.sum(pieces.reshape(2, 1, tok_dev), axis=0)
    grad_logits = router_probs * (gate_tokens - router_sum)

    return grad_tokens, grad_logits, grad_down[None], grad_up[None], gate_grad.T[None]


def solution(mesh):
    split = Mesh(mesh.devices.reshape(4, 8, mesh.shape["expert"]), (X, Y, E))
    dp = (X, Y)
    return jax.shard_map(
        local,
        mesh=split,
        in_specs=(
            P(dp, E),
            P(dp, E),
            P(E, dp),
            P(),
            P(E, None, dp),
            P(E, None, dp),
            P(E, dp, None),
            P(E, dp, None),
        ),
        out_specs=(P(dp, E), P(E, dp), P(E, dp, None), P(E, dp, None), P(E, None, dp)),
        check_vma=False,
    )
```

```python
import jax
import jax.numpy as jnp
from jax import lax
from jax.sharding import Mesh
from jax.sharding import PartitionSpec as P


X, Y, E = "dp_0", "dp_1", "expert"
BF, F32 = jnp.bfloat16, jnp.float32
PAD = 8


def exchange(x, axis):
    return lax.all_to_all(x, axis, 0, 0, tiled=True)


def dot(a, b, ca, cb):
    return lax.dot_general(a, b, (((ca,), (cb,)), ((), ())), preferred_element_type=F32)


def onehot(mask):
    return mask.astype(BF)


def rows_of(n, m):
    return lax.broadcasted_iota(jnp.int32, (n, m), 0)


def lanes_of(n, m):
    return lax.broadcasted_iota(jnp.int32, (n, m), 1)


def shift(x, by):
    size = lax.axis_size(X)
    return lax.ppermute(x, X, [(i, (i + by) % size) for i in range(size)])


def over_x(blocks, sign):
    came = [blocks[0]]
    for k in range(1, len(blocks)):
        came.append(shift(blocks[k], sign * k))
    return came


def to_quarters(x, ny):
    size = x.shape[0] * ny
    sent = jnp.broadcast_to(x[:, None], (x.shape[0], ny, *x.shape[1:]))
    return exchange(sent.reshape(size, *x.shape[1:]), (X, Y))


def joined(x, pieces):
    size, rows, lane = x.shape
    x = x.reshape(size, pieces, rows // pieces, lane).transpose(0, 2, 1, 3)
    return x.reshape(size * rows // pieces, pieces * lane)


def back_in_x(blocks, xi):
    size = blocks.shape[0]
    return [
        lax.dynamic_index_in_dim(blocks, (xi + size - k) % size, 0, keepdims=False)
        for k in range(size)
    ]


def quarter_at(w, index, nx):
    return lax.dynamic_slice_in_dim(w, index * (w.shape[1] // nx), w.shape[1] // nx, axis=1)


def in_turn(parts, xi):
    size = len(parts)
    stacked = jnp.stack(parts)
    picked = [
        lax.dynamic_index_in_dim(stacked, (q + size - xi) % size, 0, keepdims=False)
        for q in range(size)
    ]
    return jnp.concatenate(picked, axis=1)


def local(grad_out, saved_inputs, router_probs, chosen, gate_pre, up_pre, w_down, w_up):
    tok_dev, width_dev = grad_out.shape
    nx, ny, ne = lax.axis_size(X), lax.axis_size(Y), lax.axis_size(E)
    shards = nx * ny
    xi, yi, ei = lax.axis_index(X), lax.axis_index(Y), lax.axis_index(E)
    shard = xi * ny + yi
    slots = chosen.shape[1]
    cap = 3 * slots // (2 * shards)
    units = gate_pre.shape[2]
    quarter = ne // nx
    part = quarter * width_dev
    lane = width_dev

    firsts = jnp.sum((chosen < shard * tok_dev).astype(jnp.int32), axis=1)
    ends = jnp.sum((chosen < (shard + 1) * tok_dev).astype(jnp.int32), axis=1)
    offsets = jnp.arange(cap + PAD, dtype=jnp.int32)
    places = firsts[:, None] + offsets[None, :]
    live = (places < ends[:, None]) & (offsets < cap)[None, :]
    slot_iota = jnp.arange(slots, dtype=jnp.int32)
    found = jnp.sum(
        jnp.where(places[:, :, None] == slot_iota[None, None, :], chosen[:, None, :], 0), axis=2
    )
    local_rows = jnp.where(live, found - shard * tok_dev, -1)
    token_iota = jnp.arange(tok_dev, dtype=jnp.int32)
    picker = onehot(local_rows[:, :, None] == token_iota[None, None, :])

    sent_pick = picker[:, :cap].reshape(ne * cap, tok_dev)
    both = jnp.concatenate([grad_out, saved_inputs], axis=1)
    sent = dot(sent_pick, both, 1, 0).astype(BF).reshape(ne, cap, 2 * width_dev)
    rows = exchange(sent, E).reshape(nx, quarter, cap, 2 * width_dev)

    down_part = jnp.concatenate([quarter_at(w_down[0], (xi + nx - k) % nx, nx) for k in range(nx)], axis=1)
    up_part = [quarter_at(w_up[0], (xi + k) % nx, nx) for k in range(nx)]
    up_part = jnp.concatenate(over_x(up_part, 1), axis=0)

    own_rows = lax.dynamic_index_in_dim(local_rows, ei, 0, keepdims=False)
    own_rows = jnp.pad(own_rows, (0, lane - cap - PAD), constant_values=-1)
    own_hit = onehot(own_rows[:, None] == token_iota[None, :])
    gate_row = dot(router_probs.astype(BF), own_hit, 1, 1).astype(BF)
    gate_tile = jnp.broadcast_to(
        jnp.pad(gate_row, ((0, PAD - 1), (0, 0)))[None], (nx, PAD, lane)
    )
    grads = jnp.concatenate([rows[..., :lane].reshape(nx, quarter * cap, lane), gate_tile], axis=1)
    inputs = rows[..., lane:].reshape(nx, quarter * cap, lane)

    gate_value = gate_pre[0].T.astype(F32)
    up_value = up_pre[0].T.astype(F32)
    sig = jax.nn.sigmoid(gate_value)
    active = gate_value * sig
    hidden = active * up_value

    grads_all = to_quarters(grads, ny)
    inputs_all = to_quarters(inputs, ny)

    chosen_row = lax.dynamic_index_in_dim(chosen, ei, 0, keepdims=True)
    owner = chosen_row // tok_dev
    shard_col = rows_of(shards, slots)
    before = jnp.sum((owner < shard_col).astype(jnp.int32), axis=1, keepdims=True)
    within = lanes_of(1, slots) - jnp.sum(
        jnp.where(owner == shard_col, before, 0), axis=0, keepdims=True
    )
    place = onehot(rows_of(shards * cap, slots) == owner * cap + within)
    owner_hit = owner == shard_col
    within_hit = onehot(rows_of(lane, slots) == within)

    grads_slots = dot(place, joined(grads_all[:, : quarter * cap], quarter), 0, 0).astype(BF)
    gates_all = grads_all[:, quarter * cap]
    gate_slot = jnp.sum(
        jnp.where(owner_hit, dot(gates_all, within_hit, 1, 0), 0.0), axis=0, keepdims=True
    )
    grads_slots = jnp.concatenate(over_x([grads_slots] * nx, 1), axis=1)
    raw_grad = dot(down_part, grads_slots, 1, 1)
    dots = jnp.sum(hidden * raw_grad, axis=0, keepdims=True)
    hid_grad = gate_slot * raw_grad
    up_grad = (hid_grad * active).astype(BF)
    gate_grad = (hid_grad * up_value * sig * (1.0 + gate_value * (1.0 - sig))).astype(BF)
    up_all = lax.all_gather(up_grad, X)
    up_all = jnp.concatenate(back_in_x(up_all, xi), axis=0)

    hidden_gated = (hidden.astype(BF).astype(F32) * gate_slot).astype(BF)
    grad_down = dot(hidden_gated, grads_slots, 1, 0).astype(BF)
    grad_down = jnp.concatenate(
        [quarter_at(grad_down, (xi + nx - q) % nx, nx) for q in range(nx)], axis=1
    )
    dx = dot(up_all, up_part, 0, 0).astype(BF)
    dx_rows = dot(place, dx, 1, 0).astype(BF).reshape(shards, cap, quarter, lane)
    dx_rows = dx_rows.transpose(0, 2, 1, 3).reshape(shards, quarter * cap, lane)
    dots_own = jnp.where(owner_hit, dots, 0.0).astype(BF)
    dots_rows = dot(dots_own, within_hit, 1, 1).astype(BF)
    dots_rows = jnp.pad(dots_rows[:, None], ((0, 0), (0, PAD - 1), (0, 0)))
    dx_back = exchange(jnp.concatenate([dx_rows, dots_rows], axis=1), (X, Y))
    inputs_slots = dot(place, joined(inputs_all, quarter), 0, 0).astype(BF)
    grad_up = dot(up_all, inputs_slots, 1, 0).astype(BF).reshape(nx, units, part)
    up_home = over_x(grad_up, -1)
    dx_sum = jnp.sum(dx_back.reshape(nx, ny, -1, lane).astype(F32), axis=1)
    dots_sum = jnp.sum(dx_sum[:, quarter * cap], axis=0, keepdims=True)
    gate_tokens = lax.dot_general(
        dots_sum,
        own_hit.astype(F32),
        (((1,), (0,)), ((), ())),
        precision=lax.Precision.HIGHEST,
        preferred_element_type=F32,
    )
    product = router_probs * gate_tokens
    high = lax.reduce_precision(product, 8, 7)
    low = product - high
    tail = jnp.concatenate([high, low], axis=0).astype(BF).reshape(-1, lane)
    tail = jnp.pad(tail, ((0, PAD - tail.shape[0]), (0, 0)))
    to_experts = dx_sum[:, : quarter * cap].astype(BF).reshape(ne, cap, width_dev)
    spread = exchange(
        jnp.concatenate([to_experts, jnp.broadcast_to(tail[None], (ne, PAD, lane))], axis=1), E
    )
    up_home, spread = lax.optimization_barrier((up_home, spread))
    grad_up = in_turn(up_home, xi)
    grad_tokens = dot(picker.reshape(-1, tok_dev), spread.reshape(-1, width_dev), 0, 0).astype(BF)
    pieces = jnp.sum(spread[:, cap : cap + 2 * tok_dev // lane].astype(F32), axis=0)
    router_sum = jnp.sum(pieces.reshape(2, 1, tok_dev), axis=0)
    grad_logits = router_probs * (gate_tokens - router_sum)

    return grad_tokens, grad_logits, grad_down[None], grad_up[None], gate_grad.T[None]


def solution(mesh):
    split = Mesh(mesh.devices.reshape(4, 8, mesh.shape["expert"]), (X, Y, E))
    dp = (X, Y)
    return jax.shard_map(
        local,
        mesh=split,
        in_specs=(
            P(dp, E),
            P(dp, E),
            P(E, dp),
            P(),
            P(E, None, dp),
            P(E, None, dp),
            P(E, dp, None),
            P(E, dp, None),
        ),
        out_specs=(P(dp, E), P(E, dp), P(E, dp, None), P(E, dp, None), P(E, None, dp)),
        check_vma=False,
    )
```

```python
import jax
import jax.numpy as jnp
from jax import lax
from jax.sharding import Mesh
from jax.sharding import PartitionSpec as P


X, Y, E = "dp_0", "dp_1", "expert"
BF, F32 = jnp.bfloat16, jnp.float32
PAD = 8


def exchange(x, axis):
    return lax.all_to_all(x, axis, 0, 0, tiled=True)


def to_all(x, axis):
    size = lax.axis_size(axis)
    return exchange(jnp.broadcast_to(x[None], (size, *x.shape)), axis)


def dot(a, b, ca, cb):
    return lax.dot_general(a, b, (((ca,), (cb,)), ((), ())), preferred_element_type=F32)


def onehot(mask):
    return mask.astype(BF)


def rows_of(n, m):
    return lax.broadcasted_iota(jnp.int32, (n, m), 0)


def lanes_of(n, m):
    return lax.broadcasted_iota(jnp.int32, (n, m), 1)


def shift(x, by):
    size = lax.axis_size(X)
    return lax.ppermute(x, X, [(i, (i + by) % size) for i in range(size)])


def over_x(blocks, sign):
    came = [blocks[0]]
    for k in range(1, len(blocks)):
        came.append(shift(blocks[k], sign * k))
    return came


def to_quarters(x, ny):
    size = x.shape[0] * ny
    sent = jnp.broadcast_to(x[:, None], (x.shape[0], ny, *x.shape[1:]))
    return exchange(sent.reshape(size, *x.shape[1:]), (X, Y))


def joined(x, pieces):
    size, rows, lane = x.shape
    x = x.reshape(size, pieces, rows // pieces, lane).transpose(0, 2, 1, 3)
    return x.reshape(size * rows // pieces, pieces * lane)


def back_in_x(blocks, xi):
    size = blocks.shape[0]
    return [
        lax.dynamic_index_in_dim(blocks, (xi + size - k) % size, 0, keepdims=False)
        for k in range(size)
    ]


def quarter_at(w, index, nx):
    return lax.dynamic_slice_in_dim(w, index * (w.shape[1] // nx), w.shape[1] // nx, axis=1)


def in_turn(parts, xi):
    size = len(parts)
    stacked = jnp.stack(parts)
    picked = [
        lax.dynamic_index_in_dim(stacked, (q + size - xi) % size, 0, keepdims=False)
        for q in range(size)
    ]
    return jnp.concatenate(picked, axis=1)


def local(grad_out, saved_inputs, router_probs, chosen, gate_pre, up_pre, w_down, w_up):
    tok_dev, width_dev = grad_out.shape
    nx, ny, ne = lax.axis_size(X), lax.axis_size(Y), lax.axis_size(E)
    shards = nx * ny
    xi, yi, ei = lax.axis_index(X), lax.axis_index(Y), lax.axis_index(E)
    shard = xi * ny + yi
    slots = chosen.shape[1]
    cap = 3 * slots // (2 * shards)
    units = gate_pre.shape[2]
    quarter = ne // nx
    part = quarter * width_dev
    lane = width_dev

    firsts = jnp.sum((chosen < shard * tok_dev).astype(jnp.int32), axis=1)
    ends = jnp.sum((chosen < (shard + 1) * tok_dev).astype(jnp.int32), axis=1)
    offsets = jnp.arange(cap + PAD, dtype=jnp.int32)
    places = firsts[:, None] + offsets[None, :]
    live = (places < ends[:, None]) & (offsets < cap)[None, :]
    slot_iota = jnp.arange(slots, dtype=jnp.int32)
    found = jnp.sum(
        jnp.where(places[:, :, None] == slot_iota[None, None, :], chosen[:, None, :], 0), axis=2
    )
    local_rows = jnp.where(live, found - shard * tok_dev, -1)
    token_iota = jnp.arange(tok_dev, dtype=jnp.int32)
    picker = onehot(local_rows[:, :, None] == token_iota[None, None, :])

    sent_pick = picker[:, :cap].reshape(ne * cap, tok_dev)
    both = jnp.concatenate([grad_out, saved_inputs], axis=1)
    sent = dot(sent_pick, both, 1, 0).astype(BF).reshape(ne, cap, 2 * width_dev)
    rows = exchange(sent, E).reshape(nx, quarter, cap, 2 * width_dev)

    down_part = jnp.concatenate([quarter_at(w_down[0], (xi + nx - k) % nx, nx) for k in range(nx)], axis=1)
    up_part = [quarter_at(w_up[0], (xi + k) % nx, nx) for k in range(nx)]
    up_part = jnp.concatenate(over_x(up_part, 1), axis=0)

    own_rows = lax.dynamic_index_in_dim(local_rows, ei, 0, keepdims=False)
    own_rows = jnp.pad(own_rows, (0, lane - cap - PAD), constant_values=-1)
    own_hit = onehot(own_rows[:, None] == token_iota[None, :])
    gate_row = dot(router_probs.astype(BF), own_hit, 1, 1).astype(BF)
    gate_tile = jnp.broadcast_to(
        jnp.pad(gate_row, ((0, PAD - 1), (0, 0)))[None], (nx, PAD, lane)
    )
    grads = jnp.concatenate([rows[..., :lane].reshape(nx, quarter * cap, lane), gate_tile], axis=1)
    inputs = rows[..., lane:].reshape(nx, quarter * cap, lane)
    inputs = [
        lax.dynamic_index_in_dim(inputs, (xi + k) % nx, 0, keepdims=False) for k in range(nx)
    ]
    inputs = jnp.concatenate(over_x(inputs, 1), axis=0)

    gate_value = gate_pre[0].T.astype(F32)
    up_value = up_pre[0].T.astype(F32)
    sig = jax.nn.sigmoid(gate_value)
    active = gate_value * sig
    hidden = active * up_value

    grads_all = to_quarters(grads, ny)
    inputs_all = to_all(inputs, Y).reshape(shards, quarter * cap, lane)

    chosen_row = lax.dynamic_index_in_dim(chosen, ei, 0, keepdims=True)
    owner = chosen_row // tok_dev
    shard_col = rows_of(shards, slots)
    before = jnp.sum((owner < shard_col).astype(jnp.int32), axis=1, keepdims=True)
    within = lanes_of(1, slots) - jnp.sum(
        jnp.where(owner == shard_col, before, 0), axis=0, keepdims=True
    )
    place = onehot(rows_of(shards * cap, slots) == owner * cap + within)
    behind = (xi + nx - owner // ny) % nx
    place_inputs = onehot(
        rows_of(shards * cap, slots) == (owner % ny * nx + behind) * cap + within
    )
    owner_hit = owner == shard_col
    within_hit = onehot(rows_of(lane, slots) == within)

    grads_slots = dot(place, joined(grads_all[:, : quarter * cap], quarter), 0, 0).astype(BF)
    gates_all = grads_all[:, quarter * cap]
    gate_slot = jnp.sum(
        jnp.where(owner_hit, dot(gates_all, within_hit, 1, 0), 0.0), axis=0, keepdims=True
    )
    grads_slots = jnp.concatenate(over_x([grads_slots] * nx, 1), axis=1)
    raw_grad = dot(down_part, grads_slots, 1, 1)
    dots = jnp.sum(hidden * raw_grad, axis=0, keepdims=True)
    hid_grad = gate_slot * raw_grad
    up_grad = (hid_grad * active).astype(BF)
    gate_grad = (hid_grad * up_value * sig * (1.0 + gate_value * (1.0 - sig))).astype(BF)
    up_all = lax.all_gather(up_grad, X)
    up_all = jnp.concatenate(back_in_x(up_all, xi), axis=0)

    hidden_gated = (hidden.astype(BF).astype(F32) * gate_slot).astype(BF)
    grad_down = dot(hidden_gated, grads_slots, 1, 0).astype(BF)
    grad_down = jnp.concatenate(
        [quarter_at(grad_down, (xi + nx - q) % nx, nx) for q in range(nx)], axis=1
    )
    dx = dot(up_all, up_part, 0, 0).astype(BF)
    dx_rows = dot(place, dx, 1, 0).astype(BF).reshape(shards, cap, quarter, lane)
    dx_rows = dx_rows.transpose(0, 2, 1, 3).reshape(shards, quarter * cap, lane)
    dots_own = jnp.where(owner_hit, dots, 0.0).astype(BF)
    dots_rows = dot(dots_own, within_hit, 1, 1).astype(BF)
    dots_rows = jnp.pad(dots_rows[:, None], ((0, 0), (0, PAD - 1), (0, 0)))
    dx_back = exchange(jnp.concatenate([dx_rows, dots_rows], axis=1), (X, Y))
    inputs_slots = dot(place_inputs, joined(inputs_all, quarter), 0, 0).astype(BF)
    grad_up = dot(up_all, inputs_slots, 1, 0).astype(BF).reshape(nx, units, part)
    up_home = over_x(grad_up, -1)
    dx_sum = jnp.sum(dx_back.reshape(nx, ny, -1, lane).astype(F32), axis=1)
    dots_sum = jnp.sum(dx_sum[:, quarter * cap], axis=0, keepdims=True)
    gate_tokens = lax.dot_general(
        dots_sum,
        own_hit.astype(F32),
        (((1,), (0,)), ((), ())),
        precision=lax.Precision.HIGHEST,
        preferred_element_type=F32,
    )
    product = router_probs * gate_tokens
    high = lax.reduce_precision(product, 8, 7)
    low = product - high
    tail = jnp.concatenate([high, low], axis=0).astype(BF).reshape(-1, lane)
    tail = jnp.pad(tail, ((0, PAD - tail.shape[0]), (0, 0)))
    to_experts = dx_sum[:, : quarter * cap].astype(BF).reshape(ne, cap, width_dev)
    spread = exchange(
        jnp.concatenate([to_experts, jnp.broadcast_to(tail[None], (ne, PAD, lane))], axis=1), E
    )
    grad_up = in_turn(up_home, xi)
    grad_tokens = dot(picker.reshape(-1, tok_dev), spread.reshape(-1, width_dev), 0, 0).astype(BF)
    pieces = jnp.sum(spread[:, cap : cap + 2 * tok_dev // lane].astype(F32), axis=0)
    router_sum = jnp.sum(pieces.reshape(2, 1, tok_dev), axis=0)
    grad_logits = router_probs * (gate_tokens - router_sum)

    return grad_tokens, grad_logits, grad_down[None], grad_up[None], gate_grad.T[None]


def solution(mesh):
    split = Mesh(mesh.devices.reshape(4, 8, mesh.shape["expert"]), (X, Y, E))
    dp = (X, Y)
    return jax.shard_map(
        local,
        mesh=split,
        in_specs=(
            P(dp, E),
            P(dp, E),
            P(E, dp),
            P(),
            P(E, None, dp),
            P(E, None, dp),
            P(E, dp, None),
            P(E, dp, None),
        ),
        out_specs=(P(dp, E), P(E, dp), P(E, dp, None), P(E, dp, None), P(E, None, dp)),
        check_vma=False,
    )
```

```python
import jax
import jax.numpy as jnp
from jax import lax
from jax.sharding import Mesh
from jax.sharding import PartitionSpec as P


X, Y, E = "dp_0", "dp_1", "expert"
BF, F32 = jnp.bfloat16, jnp.float32
PAD = 8


def exchange(x, axis):
    return lax.all_to_all(x, axis, 0, 0, tiled=True)


def to_all(x, axis):
    size = lax.axis_size(axis)
    return exchange(jnp.broadcast_to(x[None], (size, *x.shape)), axis)


def dot(a, b, ca, cb):
    return lax.dot_general(a, b, (((ca,), (cb,)), ((), ())), preferred_element_type=F32)


def onehot(mask):
    return mask.astype(BF)


def rows_of(n, m):
    return lax.broadcasted_iota(jnp.int32, (n, m), 0)


def lanes_of(n, m):
    return lax.broadcasted_iota(jnp.int32, (n, m), 1)


def shift(x, by):
    size = lax.axis_size(X)
    return lax.ppermute(x, X, [(i, (i + by) % size) for i in range(size)])


def over_x(blocks, sign):
    came = [blocks[0]]
    for k in range(1, len(blocks)):
        came.append(shift(blocks[k], sign * k))
    return came


def to_quarters(x, ny):
    size = x.shape[0] * ny
    sent = jnp.broadcast_to(x[:, None], (x.shape[0], ny, *x.shape[1:]))
    return exchange(sent.reshape(size, *x.shape[1:]), (X, Y))


def joined(x, pieces):
    size, rows, lane = x.shape
    x = x.reshape(size, pieces, rows // pieces, lane).transpose(0, 2, 1, 3)
    return x.reshape(size * rows // pieces, pieces * lane)


def back_in_x(blocks, xi):
    size = blocks.shape[0]
    return [
        lax.dynamic_index_in_dim(blocks, (xi + size - k) % size, 0, keepdims=False)
        for k in range(size)
    ]


def quarter_at(w, index, nx):
    return lax.dynamic_slice_in_dim(w, index * (w.shape[1] // nx), w.shape[1] // nx, axis=1)


def in_turn(parts, xi):
    size = len(parts)
    stacked = jnp.stack(parts)
    picked = [
        lax.dynamic_index_in_dim(stacked, (q + size - xi) % size, 0, keepdims=False)
        for q in range(size)
    ]
    return jnp.concatenate(picked, axis=1)


def local(grad_out, saved_inputs, router_probs, chosen, gate_pre, up_pre, w_down, w_up):
    tok_dev, width_dev = grad_out.shape
    nx, ny, ne = lax.axis_size(X), lax.axis_size(Y), lax.axis_size(E)
    shards = nx * ny
    xi, yi, ei = lax.axis_index(X), lax.axis_index(Y), lax.axis_index(E)
    shard = xi * ny + yi
    slots = chosen.shape[1]
    cap = 3 * slots // (2 * shards)
    units = gate_pre.shape[2]
    quarter = ne // nx
    part = quarter * width_dev
    lane = width_dev

    firsts = jnp.sum((chosen < shard * tok_dev).astype(jnp.int32), axis=1)
    ends = jnp.sum((chosen < (shard + 1) * tok_dev).astype(jnp.int32), axis=1)
    offsets = jnp.arange(cap + PAD, dtype=jnp.int32)
    places = firsts[:, None] + offsets[None, :]
    live = (places < ends[:, None]) & (offsets < cap)[None, :]
    slot_iota = jnp.arange(slots, dtype=jnp.int32)
    found = jnp.sum(
        jnp.where(places[:, :, None] == slot_iota[None, None, :], chosen[:, None, :], 0), axis=2
    )
    local_rows = jnp.where(live, found - shard * tok_dev, -1)
    token_iota = jnp.arange(tok_dev, dtype=jnp.int32)
    picker = onehot(local_rows[:, :, None] == token_iota[None, None, :])

    sent_pick = picker[:, :cap].reshape(ne * cap, tok_dev)
    both = jnp.concatenate([grad_out, saved_inputs], axis=1)
    sent = dot(sent_pick, both, 1, 0).astype(BF).reshape(ne, cap, 2 * width_dev)
    rows = exchange(sent, E).reshape(nx, quarter, cap, 2 * width_dev)

    down_part = jnp.concatenate([quarter_at(w_down[0], (xi + nx - k) % nx, nx) for k in range(nx)], axis=1)
    up_part = [quarter_at(w_up[0], (xi + k) % nx, nx) for k in range(nx)]
    up_part = over_x(up_part, 1)
    up_part = jnp.concatenate(back_in_x(jnp.stack(up_part), xi), axis=0)

    own_rows = lax.dynamic_index_in_dim(local_rows, ei, 0, keepdims=False)
    own_rows = jnp.pad(own_rows, (0, lane - cap - PAD), constant_values=-1)
    own_hit = onehot(own_rows[:, None] == token_iota[None, :])
    gate_row = dot(router_probs.astype(BF), own_hit, 1, 1).astype(BF)
    gate_tile = jnp.broadcast_to(
        jnp.pad(gate_row, ((0, PAD - 1), (0, 0)))[None], (nx, PAD, lane)
    )
    grads = jnp.concatenate([rows[..., :lane].reshape(nx, quarter * cap, lane), gate_tile], axis=1)
    inputs = rows[..., lane:].reshape(nx, quarter * cap, lane)
    inputs = [
        lax.dynamic_index_in_dim(inputs, (xi + k) % nx, 0, keepdims=False) for k in range(nx)
    ]
    inputs = jnp.concatenate(over_x(inputs, 1), axis=0)

    gate_value = gate_pre[0].T.astype(F32)
    up_value = up_pre[0].T.astype(F32)
    sig = jax.nn.sigmoid(gate_value)
    active = gate_value * sig
    hidden = active * up_value

    grads_all = to_quarters(grads, ny)
    inputs_all = to_all(inputs, Y).reshape(shards, quarter * cap, lane)

    chosen_row = lax.dynamic_index_in_dim(chosen, ei, 0, keepdims=True)
    owner = chosen_row // tok_dev
    shard_col = rows_of(shards, slots)
    before = jnp.sum((owner < shard_col).astype(jnp.int32), axis=1, keepdims=True)
    within = lanes_of(1, slots) - jnp.sum(
        jnp.where(owner == shard_col, before, 0), axis=0, keepdims=True
    )
    place = onehot(rows_of(shards * cap, slots) == owner * cap + within)
    behind = (xi + nx - owner // ny) % nx
    place_inputs = onehot(
        rows_of(shards * cap, slots) == (owner % ny * nx + behind) * cap + within
    )
    owner_hit = owner == shard_col
    within_hit = onehot(rows_of(lane, slots) == within)

    grads_slots = dot(place, joined(grads_all[:, : quarter * cap], quarter), 0, 0).astype(BF)
    gates_all = grads_all[:, quarter * cap]
    gate_slot = jnp.sum(
        jnp.where(owner_hit, dot(gates_all, within_hit, 1, 0), 0.0), axis=0, keepdims=True
    )
    grads_slots = jnp.concatenate(over_x([grads_slots] * nx, 1), axis=1)
    raw_grad = dot(down_part, grads_slots, 1, 1)
    dots = jnp.sum(hidden * raw_grad, axis=0, keepdims=True)
    hid_grad = gate_slot * raw_grad
    up_grad = (hid_grad * active).astype(BF)
    gate_grad = (hid_grad * up_value * sig * (1.0 + gate_value * (1.0 - sig))).astype(BF)
    up_all = lax.all_gather(up_grad, X)
    up_all = up_all.reshape(nx * units, slots)

    hidden_gated = (hidden.astype(BF).astype(F32) * gate_slot).astype(BF)
    grad_down = dot(hidden_gated, grads_slots, 1, 0).astype(BF)
    grad_down = jnp.concatenate(
        [quarter_at(grad_down, (xi + nx - q) % nx, nx) for q in range(nx)], axis=1
    )
    dx = dot(up_all, up_part, 0, 0).astype(BF)
    dx_rows = dot(place, dx, 1, 0).astype(BF).reshape(shards, cap, quarter, lane)
    dx_rows = dx_rows.transpose(0, 2, 1, 3).reshape(shards, quarter * cap, lane)
    dots_own = jnp.where(owner_hit, dots, 0.0).astype(BF)
    dots_rows = dot(dots_own, within_hit, 1, 1).astype(BF)
    dots_rows = jnp.pad(dots_rows[:, None], ((0, 0), (0, PAD - 1), (0, 0)))
    dx_back = exchange(jnp.concatenate([dx_rows, dots_rows], axis=1), (X, Y))
    inputs_slots = dot(place_inputs, joined(inputs_all, quarter), 0, 0).astype(BF)
    grad_up = dot(up_all, inputs_slots, 1, 0).astype(BF).reshape(nx, units, part)
    up_home = over_x(back_in_x(grad_up, xi), -1)
    dx_sum = jnp.sum(dx_back.reshape(nx, ny, -1, lane).astype(F32), axis=1)
    dots_sum = jnp.sum(dx_sum[:, quarter * cap], axis=0, keepdims=True)
    gate_tokens = lax.dot_general(
        dots_sum,
        own_hit.astype(F32),
        (((1,), (0,)), ((), ())),
        precision=lax.Precision.HIGHEST,
        preferred_element_type=F32,
    )
    product = router_probs * gate_tokens
    high = lax.reduce_precision(product, 8, 7)
    low = product - high
    tail = jnp.concatenate([high, low], axis=0).astype(BF).reshape(-1, lane)
    tail = jnp.pad(tail, ((0, PAD - tail.shape[0]), (0, 0)))
    to_experts = dx_sum[:, : quarter * cap].astype(BF).reshape(ne, cap, width_dev)
    spread = exchange(
        jnp.concatenate([to_experts, jnp.broadcast_to(tail[None], (ne, PAD, lane))], axis=1), E
    )
    grad_up = in_turn(up_home, xi)
    grad_tokens = dot(picker.reshape(-1, tok_dev), spread.reshape(-1, width_dev), 0, 0).astype(BF)
    pieces = jnp.sum(spread[:, cap : cap + 2 * tok_dev // lane].astype(F32), axis=0)
    router_sum = jnp.sum(pieces.reshape(2, 1, tok_dev), axis=0)
    grad_logits = router_probs * (gate_tokens - router_sum)

    return grad_tokens, grad_logits, grad_down[None], grad_up[None], gate_grad.T[None]


def solution(mesh):
    split = Mesh(mesh.devices.reshape(4, 8, mesh.shape["expert"]), (X, Y, E))
    dp = (X, Y)
    return jax.shard_map(
        local,
        mesh=split,
        in_specs=(
            P(dp, E),
            P(dp, E),
            P(E, dp),
            P(),
            P(E, None, dp),
            P(E, None, dp),
            P(E, dp, None),
            P(E, dp, None),
        ),
        out_specs=(P(dp, E), P(E, dp), P(E, dp, None), P(E, dp, None), P(E, None, dp)),
        check_vma=False,
    )
```

```python
import jax
import jax.numpy as jnp
from jax import lax
from jax.sharding import Mesh
from jax.sharding import PartitionSpec as P


X, Y, E = "dp_0", "dp_1", "expert"
BF, F32 = jnp.bfloat16, jnp.float32
PAD = 8


def exchange(x, axis):
    return lax.all_to_all(x, axis, 0, 0, tiled=True)


def to_all(x, axis):
    size = lax.axis_size(axis)
    return exchange(jnp.broadcast_to(x[None], (size, *x.shape)), axis)


def dot(a, b, ca, cb):
    return lax.dot_general(a, b, (((ca,), (cb,)), ((), ())), preferred_element_type=F32)


def onehot(mask):
    return mask.astype(BF)


def rows_of(n, m):
    return lax.broadcasted_iota(jnp.int32, (n, m), 0)


def lanes_of(n, m):
    return lax.broadcasted_iota(jnp.int32, (n, m), 1)


def shift(x, by):
    size = lax.axis_size(X)
    return lax.ppermute(x, X, [(i, (i + by) % size) for i in range(size)])


def over_x(blocks, sign):
    came = [blocks[0]]
    for k in range(1, len(blocks)):
        came.append(shift(blocks[k], sign * k))
    return came


def to_quarters(x, ny):
    size = x.shape[0] * ny
    sent = jnp.broadcast_to(x[:, None], (x.shape[0], ny, *x.shape[1:]))
    return exchange(sent.reshape(size, *x.shape[1:]), (X, Y))


def joined(x, pieces):
    size, rows, lane = x.shape
    x = x.reshape(size, pieces, rows // pieces, lane).transpose(0, 2, 1, 3)
    return x.reshape(size * rows // pieces, pieces * lane)


def back_in_x(blocks, xi):
    size = blocks.shape[0]
    return [
        lax.dynamic_index_in_dim(blocks, (xi + size - k) % size, 0, keepdims=False)
        for k in range(size)
    ]


def quarter_at(w, index, nx):
    return lax.dynamic_slice_in_dim(w, index * (w.shape[1] // nx), w.shape[1] // nx, axis=1)


def in_turn(parts, xi):
    size = len(parts)
    stacked = jnp.stack(parts)
    picked = [
        lax.dynamic_index_in_dim(stacked, (q + size - xi) % size, 0, keepdims=False)
        for q in range(size)
    ]
    return jnp.concatenate(picked, axis=1)


def local(grad_out, saved_inputs, router_probs, chosen, gate_pre, up_pre, w_down, w_up):
    tok_dev, width_dev = grad_out.shape
    nx, ny, ne = lax.axis_size(X), lax.axis_size(Y), lax.axis_size(E)
    shards = nx * ny
    xi, yi, ei = lax.axis_index(X), lax.axis_index(Y), lax.axis_index(E)
    shard = xi * ny + yi
    slots = chosen.shape[1]
    cap = 3 * slots // (2 * shards)
    units = gate_pre.shape[2]
    quarter = ne // nx
    part = quarter * width_dev
    lane = width_dev

    firsts = jnp.sum((chosen < shard * tok_dev).astype(jnp.int32), axis=1)
    ends = jnp.sum((chosen < (shard + 1) * tok_dev).astype(jnp.int32), axis=1)
    offsets = jnp.arange(cap + PAD, dtype=jnp.int32)
    places = firsts[:, None] + offsets[None, :]
    live = (places < ends[:, None]) & (offsets < cap)[None, :]
    slot_iota = jnp.arange(slots, dtype=jnp.int32)
    found = jnp.sum(
        jnp.where(places[:, :, None] == slot_iota[None, None, :], chosen[:, None, :], 0), axis=2
    )
    local_rows = jnp.where(live, found - shard * tok_dev, -1)
    token_iota = jnp.arange(tok_dev, dtype=jnp.int32)
    picker = onehot(local_rows[:, :, None] == token_iota[None, None, :])

    sent_pick = picker[:, :cap].reshape(ne * cap, tok_dev)
    both = jnp.concatenate([grad_out, saved_inputs], axis=1)
    sent = dot(sent_pick, both, 1, 0).astype(BF).reshape(ne, cap, 2 * width_dev)
    rows = exchange(sent, E).reshape(nx, quarter, cap, 2 * width_dev)

    down_part = [quarter_at(w_down[0], (xi + nx - k) % nx, nx) for k in range(nx)]
    down_near = jnp.concatenate(down_part[:-1], axis=1)
    up_part = [quarter_at(w_up[0], (xi + k) % nx, nx) for k in range(nx)]
    up_part = over_x(up_part, 1)
    up_part = jnp.concatenate(back_in_x(jnp.stack(up_part), xi), axis=0)

    own_rows = lax.dynamic_index_in_dim(local_rows, ei, 0, keepdims=False)
    own_rows = jnp.pad(own_rows, (0, lane - cap - PAD), constant_values=-1)
    own_hit = onehot(own_rows[:, None] == token_iota[None, :])
    gate_row = dot(router_probs.astype(BF), own_hit, 1, 1).astype(BF)
    gate_tile = jnp.broadcast_to(
        jnp.pad(gate_row, ((0, PAD - 1), (0, 0)))[None], (nx, PAD, lane)
    )
    grads = jnp.concatenate([rows[..., :lane].reshape(nx, quarter * cap, lane), gate_tile], axis=1)
    inputs = rows[..., lane:].reshape(nx, quarter * cap, lane)
    inputs = [
        lax.dynamic_index_in_dim(inputs, (xi + k) % nx, 0, keepdims=False) for k in range(nx)
    ]
    inputs = jnp.concatenate(over_x(inputs, 1), axis=0)

    gate_value = gate_pre[0].T.astype(F32)
    up_value = up_pre[0].T.astype(F32)
    sig = jax.nn.sigmoid(gate_value)
    active = gate_value * sig
    hidden = active * up_value

    grads_all = to_quarters(grads, ny)
    inputs_all = to_all(inputs, Y).reshape(shards, quarter * cap, lane)

    chosen_row = lax.dynamic_index_in_dim(chosen, ei, 0, keepdims=True)
    owner = chosen_row // tok_dev
    shard_col = rows_of(shards, slots)
    before = jnp.sum((owner < shard_col).astype(jnp.int32), axis=1, keepdims=True)
    within = lanes_of(1, slots) - jnp.sum(
        jnp.where(owner == shard_col, before, 0), axis=0, keepdims=True
    )
    place = onehot(rows_of(shards * cap, slots) == owner * cap + within)
    behind = (xi + nx - owner // ny) % nx
    place_inputs = onehot(
        rows_of(shards * cap, slots) == (owner % ny * nx + behind) * cap + within
    )
    owner_hit = owner == shard_col
    within_hit = onehot(rows_of(lane, slots) == within)

    grads_slots = dot(place, joined(grads_all[:, : quarter * cap], quarter), 0, 0).astype(BF)
    gates_all = grads_all[:, quarter * cap]
    gate_slot = jnp.sum(
        jnp.where(owner_hit, dot(gates_all, within_hit, 1, 0), 0.0), axis=0, keepdims=True
    )
    grads_slots = over_x([grads_slots] * nx, 1)
    raw_near = dot(down_near, jnp.concatenate(grads_slots[:-1], axis=1), 1, 1)
    raw_grad = lax.optimization_barrier(raw_near) + dot(down_part[-1], grads_slots[-1], 1, 1)
    grads_slots = jnp.concatenate(grads_slots, axis=1)
    dots = jnp.sum(hidden * raw_grad, axis=0, keepdims=True)
    hid_grad = gate_slot * raw_grad
    up_grad = (hid_grad * active).astype(BF)
    gate_grad = (hid_grad * up_value * sig * (1.0 + gate_value * (1.0 - sig))).astype(BF)
    up_all = lax.all_gather(up_grad, X)
    up_all = up_all.reshape(nx * units, slots)

    hidden_gated = (hidden.astype(BF).astype(F32) * gate_slot).astype(BF)
    grad_down = dot(hidden_gated, grads_slots, 1, 0).astype(BF)
    grad_down = jnp.concatenate(
        [quarter_at(grad_down, (xi + nx - q) % nx, nx) for q in range(nx)], axis=1
    )
    dx = dot(up_all, up_part, 0, 0).astype(BF)
    dx_rows = dot(place, dx, 1, 0).astype(BF).reshape(shards, cap, quarter, lane)
    dx_rows = dx_rows.transpose(0, 2, 1, 3).reshape(shards, quarter * cap, lane)
    dots_own = jnp.where(owner_hit, dots, 0.0).astype(BF)
    dots_rows = dot(dots_own, within_hit, 1, 1).astype(BF)
    dots_rows = jnp.pad(dots_rows[:, None], ((0, 0), (0, PAD - 1), (0, 0)))
    dx_back = exchange(jnp.concatenate([dx_rows, dots_rows], axis=1), (X, Y))
    inputs_slots = dot(place_inputs, joined(inputs_all, quarter), 0, 0).astype(BF)
    grad_up = dot(up_all, inputs_slots, 1, 0).astype(BF).reshape(nx, units, part)
    up_home = over_x(back_in_x(grad_up, xi), -1)
    dx_sum = jnp.sum(dx_back.reshape(nx, ny, -1, lane).astype(F32), axis=1)
    dots_sum = jnp.sum(dx_sum[:, quarter * cap], axis=0, keepdims=True)
    gate_tokens = lax.dot_general(
        dots_sum,
        own_hit.astype(F32),
        (((1,), (0,)), ((), ())),
        precision=lax.Precision.HIGHEST,
        preferred_element_type=F32,
    )
    product = router_probs * gate_tokens
    high = lax.reduce_precision(product, 8, 7)
    low = product - high
    tail = jnp.concatenate([high, low], axis=0).astype(BF).reshape(-1, lane)
    tail = jnp.pad(tail, ((0, PAD - tail.shape[0]), (0, 0)))
    to_experts = dx_sum[:, : quarter * cap].astype(BF).reshape(ne, cap, width_dev)
    spread = exchange(
        jnp.concatenate([to_experts, jnp.broadcast_to(tail[None], (ne, PAD, lane))], axis=1), E
    )
    grad_up = in_turn(up_home, xi)
    grad_tokens = dot(picker.reshape(-1, tok_dev), spread.reshape(-1, width_dev), 0, 0).astype(BF)
    pieces = jnp.sum(spread[:, cap : cap + 2 * tok_dev // lane].astype(F32), axis=0)
    router_sum = jnp.sum(pieces.reshape(2, 1, tok_dev), axis=0)
    grad_logits = router_probs * (gate_tokens - router_sum)

    return grad_tokens, grad_logits, grad_down[None], grad_up[None], gate_grad.T[None]


def solution(mesh):
    split = Mesh(mesh.devices.reshape(4, 8, mesh.shape["expert"]), (X, Y, E))
    dp = (X, Y)
    return jax.shard_map(
        local,
        mesh=split,
        in_specs=(
            P(dp, E),
            P(dp, E),
            P(E, dp),
            P(),
            P(E, None, dp),
            P(E, None, dp),
            P(E, dp, None),
            P(E, dp, None),
        ),
        out_specs=(P(dp, E), P(E, dp), P(E, dp, None), P(E, dp, None), P(E, None, dp)),
        check_vma=False,
    )
```
